256 devices in a mesh: pipe: 8 (over y, z_lo), expert: 32 (over z_hi, x, core).
Axes of the slice: x: 4, y: 4, z: 8 (z_hi: 4, z_lo: 2; z = z_hi * 2 + z_lo), core: 2. Of those that a mesh axis runs over, the one named last changes fastest.
Arguments:
- acts: bfloat16 [8, 4096, 3584], P('pipe', 'expert'), may hold values from -6 to 6
- routes: int32 [3, 8, 4096, 8], P(None, 'pipe', 'expert'), may hold values from 0 to 255, all different within a row
- gates: float32 [3, 8, 4096, 8], P(None, 'pipe', 'expert'), may hold values from 0.1 to 1
- norm_gain: float32 [2, 8, 3584], P(None, 'pipe'), may hold values from 0.1 to 1.9
- gate_weight: bfloat16 [2, 8, 3584, 8192], P(None, 'pipe', None, 'expert'), may hold values from -0.09375 to 0.09375
- up_weight: bfloat16 [2, 8, 3584, 8192], P(None, 'pipe', None, 'expert'), may hold values from -0.09375 to 0.09375
- down_weight: bfloat16 [2, 8, 8192, 3584], P(None, 'pipe', 'expert'), may hold values from -0.125 to 0.125
Outputs:
- acts_out: bfloat16 [8, 4096, 3584], P('pipe', 'expert')
The draws below stay inside these ranges and needn't reach their ends.
Inputs may be any that keep to these rules, and one draw needn't show every extreme that they name: `routes`: each token names 8 different expert ids; only ids below 4 act in this window.
All inputs are finite; a program needn't handle non-finite values.
Results may differ from the reference program's by a relative error of at most 0.0034.
Values may be sent and summed in bfloat16 or wider, within the bound.
A program may use at most 64 MiB of HBM per device.

```python
import jax
import jax.numpy as jnp
from jax import lax

D = 3584
FE = 2048
EXPERTS_ALL = 256
TOPK = 8
SLICES = 8
CAP = 8
VIRTUAL = 2
TOK_DEV = 128
TICKS = 3
TOKG = 4096
EXP_FLIGHT = 4
N_PIPE = 8


def steps_of(own_key, shape, shards, least, high):
    def one(position, shards_of):
        draws = jax.random.uniform(jax.random.fold_in(jax.random.fold_in(own_key, 6), position), (shards_of,), jnp.float32, least / len(shards), high / len(shards))
        return jnp.repeat(jnp.exp(draws), shape[position] // shards_of).reshape((-1,) + (1,) * (len(shape) - position - 1))

    loudness = one(*shards[0])
    for cut in shards[1:]:
        loudness = loudness * one(*cut)
    return loudness


def different_ones(rng, rows, number_of, top, lift):
    sequence = jax.random.permutation(jax.random.fold_in(rng, 1), number_of)
    boost = sequence
    for power in range(3):
        boost = boost * boost // number_of
    boost = boost * lift // number_of
    lots = jax.random.randint(jax.random.fold_in(rng, 2), (rows, number_of), 0, 4096) + boost
    holders = jax.random.permutation(jax.random.fold_in(rng, 3), rows)[jnp.arange(number_of) % rows]
    lots = jnp.where(jnp.arange(rows)[:, None] == holders[None, :], 1 << 14, lots)
    priority = lots * number_of + jnp.arange(number_of)
    return lax.top_k(priority.astype(jnp.int32), top)[1].astype(jnp.int32)


def normal_values(stream_key, dims, spread, most, split=(), held_as=jnp.bfloat16):
    level = steps_of(stream_key, dims, split, -0.22, 0.18) if split else 1.0
    entries = jax.random.normal(stream_key, dims, jnp.float32) * spread * level
    return jnp.minimum(jnp.maximum(entries, -most), most).astype(held_as)


def setup_inputs(seed: int = 0) -> dict:
    seeds = jax.random.split(jax.random.key(seed), 8)
    return {
        "acts": normal_values(seeds[0], (N_PIPE, TOKG, D), 1.0, 6.0, ((0, 8), (1, 32))),
        "routes": different_ones(seeds[1], TICKS * N_PIPE * TOKG, EXPERTS_ALL, TOPK, 512).reshape((TICKS, N_PIPE, TOKG, TOPK)),
        "gates": jnp.clip(0.1 + 0.9 * jax.random.uniform(seeds[2], (TICKS, N_PIPE, TOKG, TOPK), jnp.float32) ** steps_of(seeds[2], (TICKS, N_PIPE, TOKG, TOPK), ((1, 8), (2, 32)), -0.2, 0.2), 0.1, 1.0),
        "norm_gain": jnp.clip(1.0 + 0.18 * jax.random.normal(seeds[3], (VIRTUAL, N_PIPE, D), jnp.float32), 0.1, 1.9),
        "gate_weight": normal_values(seeds[4], (VIRTUAL, N_PIPE, D, EXP_FLIGHT * FE), D ** -0.5, 0.09375, ((1, 8), (3, 32))),
        "up_weight": normal_values(seeds[5], (VIRTUAL, N_PIPE, D, EXP_FLIGHT * FE), D ** -0.5, 0.09375, ((1, 8), (3, 32))),
        "down_weight": normal_values(seeds[6], (VIRTUAL, N_PIPE, EXP_FLIGHT * FE, D), FE ** -0.5, 0.125, ((1, 8), (2, 32))),
    }


epsilon = 1e-06

def normalize(tokens_in, gain_row):
    x_float = tokens_in.astype(jnp.float32)
    inverse = lax.rsqrt(lax.optimization_barrier(jnp.mean(x_float * x_float, axis=-1, keepdims=True)) + epsilon)
    return (x_float, (x_float * inverse * gain_row).astype(jnp.bfloat16))

def moe_layer(tokens_in, route_ids, gate_values, gain_row, w_gate, w_up, w_down):
    x_float, normed = normalize(tokens_in, gain_row)
    blocks = TOKG // TOK_DEV
    hidden_dev = FE // SLICES
    normed_blocks = normed.reshape(blocks, TOK_DEV, D).astype(jnp.float32)
    output = x_float.reshape(blocks, TOK_DEV, D)
    slot_ids = jnp.arange(CAP, dtype=jnp.int32)
    for expert in range(EXP_FLIGHT):
        matches = route_ids == expert
        taken_count = lax.optimization_barrier(jnp.sum(matches.astype(jnp.int32), axis=1)).reshape(blocks, TOK_DEV)
        weight = lax.optimization_barrier(jnp.sum(jnp.where(matches, gate_values, jnp.float32(0.0)), axis=1)).reshape(blocks, TOK_DEV)
        before = jnp.cumsum(taken_count, axis=1) - taken_count
        kept_mask = taken_count * (before < CAP).astype(jnp.int32)
        placing = (kept_mask[:, :, None] * (before[:, :, None] == slot_ids[None, None, :]).astype(jnp.int32)).astype(jnp.float32)
        packed = jnp.einsum('btc,btd->bcd', placing, normed_blocks).astype(jnp.bfloat16).reshape(blocks * CAP, D)
        gate_part = jnp.dot(packed, w_gate[:, expert * FE:(expert + 1) * FE], preferred_element_type=jnp.float32)
        up_part = jnp.dot(packed, w_up[:, expert * FE:(expert + 1) * FE], preferred_element_type=jnp.float32)
        hidden = (jax.nn.silu(gate_part) * up_part).astype(jnp.bfloat16)
        down_rows = w_down[expert * FE:(expert + 1) * FE].reshape(SLICES, hidden_dev, D).astype(jnp.float32)
        pieces = jnp.einsum('rsh,shd->srd', hidden.reshape(blocks * CAP, SLICES, hidden_dev).astype(jnp.float32), down_rows)
        pieces = lax.optimization_barrier(pieces.astype(jnp.bfloat16)).astype(jnp.float32)
        expert_sum = lax.optimization_barrier(jnp.sum(pieces, axis=0)).astype(jnp.bfloat16)
        expert_out = lax.optimization_barrier(expert_sum).astype(jnp.float32).reshape(blocks, CAP, D)
        mixing = placing * weight[:, :, None]
        output = output + jnp.einsum('btc,bcd->btd', mixing, expert_out, precision=lax.Precision.HIGHEST)
    return output.reshape(TOKG, D).astype(jnp.bfloat16)

def reference(acts, routes, gates, norm_gain, gate_weight, up_weight, down_weight):
    states = [acts[microbatch] for microbatch in range(N_PIPE)]
    for moment in range(TICKS):
        for microbatch in range(N_PIPE):
            holder = (microbatch + moment) % N_PIPE
            virtual = (microbatch + moment) // N_PIPE
            states[microbatch] = moe_layer(states[microbatch], routes[moment, holder], gates[moment, holder], norm_gain[virtual, holder], gate_weight[virtual, holder], up_weight[virtual, holder], down_weight[virtual, holder])
    return jnp.stack([states[(holder - TICKS) % N_PIPE] for holder in range(N_PIPE)])
```

```python
import jax
import jax.numpy as jnp
from jax import lax
from jax.experimental import pallas as pl
from jax.experimental.pallas import tpu as pltpu
from jax.sharding import PartitionSpec as P

CAP = 8
EXPERTS = 4
NP = 8
NZ = 4
NX = 4
D = 3584
H = 2
DH = D // H
TOK = 128
HID = 256
TICKS = 3
DORD = (0, 1, 2, 3)
CROSS = (0, 0, 0)
DIRECT = 1
SLOTS = EXPERTS * CAP
epsilon = 1e-06
F32 = jnp.float32
BF16 = jnp.bfloat16
MESH = pl.DeviceIdType.MESH
NT = (((1,), (1,)), ((), ()))


def kernel(
    acts, routes, gates, gain, gw, uw, dw, out,
    x0, x1, xs, xs2, x3, ga, gb, gc, mt, tab_a, tab_b, tab_c,
    wg, wu, wd, ag, zs, rw, pre, acc, hid, pf, s1, s1r, s2, s2r, plain, plainr, eob, ret,
    in_sem, w_sem, wp_ssem, wp_rsem, t_ssem, t_rsem, b_ssem, b_rsem,
    x_ssem, z_ssem, z_rsem, xl_rsem, xr_rsem, rl_rsem, rr_rsem, a_rsem, c_rsem, d_rsem, e_rsem, p_rsem, q_rsem, v_rsem, u_rsem, r_rsem,
):
    p = lax.axis_index("pipe")
    q = lax.axis_index("expert")
    z = q // 8
    x = lax.rem(q // 2, NX)
    c = lax.rem(q, 2)
    odd = lax.rem(p, 2)

    def dev(dp, zz, xx, cc):
        return {"pipe": lax.rem(p + dp, NP), "expert": zz * 8 + xx * 2 + cc}

    def same(dp):
        return dev(dp, z, x, c)

    def other(t):
        return 1 - c if CROSS[t] else c

    near = NZ - DIRECT
    partner = dev(0, z, x, 1 - c)
    right = dev(0, z, lax.rem(x + 1, NX), c)
    left = dev(0, z, lax.rem(x + 3, NX), c)
    across = dev(0, z, lax.rem(x + 2, NX), c)

    def rc(src, dst, ss, rs, to):
        return pltpu.make_async_remote_copy(
            src_ref=src, dst_ref=dst, send_sem=ss, recv_sem=rs, device_id=to, device_id_type=MESH
        )

    def send(src, dst, ss, rs, to):
        rc(src, dst, ss, rs, to).start()

    def got(ref, sem):
        rc(ref, ref, sem, sem, right).wait_recv()

    def sent(ref, sem):
        rc(ref, ref, sem, sem, right).wait_send()

    def each(body):
        lax.fori_loop(0, H, lambda h, carry: (body(h), carry)[1], 0)

    def cols(h):
        return pl.ds(pl.multiple_of(h * DH, 128), DH)

    def z_even(offset):
        return lax.rem(z + offset, NZ)

    def z_next(k):
        if k == 0 or k == 3:
            return lax.rem(z + (0, 0, 0, 2)[k], NZ)
        return lax.rem(z + (2 * odd + 3 if k == 1 else 5 - 2 * odd), NZ)

    def dst_z(t, k):
        return z_next(k) if t == 1 else z_even((0, 1, 3, 2)[k])

    def home_z(t, k):
        return z_next(k) if t == 1 else z_even((0, 3, 1, 2)[k])

    barrier = pltpu.get_barrier_semaphore()
    flows = {(dp, cross) for t, pair in enumerate(((0, 2), (7, 1), (0, 1))) for dp in pair for cross in (CROSS[t],)}
    flows |= {((NP - dp) % NP, cross) for dp, cross in flows}
    places = {(dp, dz, cross) for dp, cross in flows for dz in range(NZ)} | {(dp, 0, 0) for dp in (1, 2, 6, 7)}
    places = sorted(places - {(0, 0, 0)} | {(0, 0, 1)})
    peers = [right, left, across] + [dev(dp, lax.rem(z + dz, NZ), x, 1 - c if cross else c) for dp, dz, cross in places]
    for peer in peers:
        pl.semaphore_signal(barrier, inc=1, device_id=peer, device_id_type=MESH)

    v1 = (8 - p) // 8
    v2 = (9 - p) // 8

    each(lambda h: pltpu.make_async_copy(acts.at[0, :, cols(h)], x0.at[h], in_sem.at[0]).start())
    pltpu.make_async_copy(gain.at[0], ga, in_sem.at[1]).start()
    pltpu.make_async_copy(gain.at[v2], gc, in_sem.at[2]).start()
    mats = ((gw, wg), (uw, wu), (dw, wd))
    earlier = (
        lax.broadcasted_iota(jnp.int32, (TOK, TOK), 0) < lax.broadcasted_iota(jnp.int32, (TOK, TOK), 1)
    ).astype(F32).astype(BF16)
    slot = lax.broadcasted_iota(jnp.int32, (CAP, TOK), 0).astype(F32)

    def table(t, carry):
        ids, values = routes[t, 0], gates[t, 0]
        taken, weight = [], []
        for e in range(EXPERTS):
            match = ids == e
            taken.append(jnp.sum(jnp.where(match, F32(1.0), F32(0.0)), axis=0, keepdims=True))
            weight.append(jnp.sum(jnp.where(match, values, F32(0.0)), axis=0, keepdims=True))
        four = jnp.concatenate(taken + [jnp.zeros((4, TOK), F32)], axis=0)
        before = jnp.dot(four.astype(BF16), earlier, preferred_element_type=F32)
        for e in range(EXPERTS):
            here = (before[e:e + 1] == slot) & (taken[e] > 0.5)
            mt[t, e * CAP:(e + 1) * CAP] = jnp.where(here, weight[e], F32(0.0))
        return carry

    lax.fori_loop(0, TICKS, table, 0)

    def chosen(tab):
        return (tab > 0).astype(F32).astype(BF16)

    def halves(tab):
        high = tab.astype(BF16).astype(F32)
        return high, tab - high

    def mixer(tab):
        high, low = halves(tab)
        return jnp.concatenate([high, low, jnp.zeros((64, TOK), F32)], axis=0).T.astype(BF16)

    def returned(t, h):
        return ret[t, :, h].astype(F32).reshape(SLOTS, DH)

    def dispatch(t, gref, dp, local):
        total = jnp.zeros((SLOTS, 1), F32)
        for h in range(H):
            total += jnp.sum(rw[h] * rw[h], axis=-1, keepdims=True)
        inverse = lax.rsqrt(total / D + epsilon)

        def scale(h):
            rows = (rw[h] * inverse * gref[:, cols(h)]).reshape(EXPERTS, CAP, DH).astype(BF16)
            zs[t, :, h] = rows

        each(scale)

        def go():
            for k in DORD:
                if not (local and k == 0):
                    zz = dst_z(t, k)
                    send(zs.at[t, zz], ag.at[t, :, 0, k], z_ssem.at[t], z_rsem.at[t, k], dev(dp, zz, x, other(t)))
            if local:
                for h in range(H):
                    ag[t, h, 0, 0] = zs[t, z, h]
        return go

    def expert(t, sel, local, home, before_first, after_first, before_end):
        def first(k):
            if not (local and k == 0):
                got(ag.at[t, :, 0, k], z_rsem.at[t, k])
            if k >= near:
                send(ag.at[t, :, 0, k], ag.at[t, :, 3, k], x_ssem.at[11], v_rsem.at[t % 2, k], across)
            send(ag.at[t, :, 0, k], ag.at[t, :, 1, k], x_ssem.at[0], xl_rsem.at[t % 2, k], right)
            send(ag.at[t, :, 0, k], ag.at[t, :, 2, k], x_ssem.at[1], xr_rsem.at[t % 2, k], left)

        def relay(k):
            got(ag.at[t, :, 1, k], xl_rsem.at[t % 2, k])
            if k < near:
                send(ag.at[t, 0, 1, k], ag.at[t, 0, 3, k], x_ssem.at[2], rl_rsem.at[t % 2], right)
            got(ag.at[t, :, 2, k], xr_rsem.at[t % 2, k])
            if k < near:
                send(ag.at[t, 1, 2, k], ag.at[t, 1, 3, k], x_ssem.at[3], rr_rsem.at[t % 2], left)
            else:
                got(ag.at[t, :, 3, k], v_rsem.at[t % 2, k])

        before_first()
        first(0)
        after_first()
        first(1)
        first(2)
        relay(0)
        first(3)
        relay(1)
        relay(2)
        relay(3)

        if t == 0:
            for i, (src, dst) in enumerate(mats[:2]):
                pltpu.make_async_copy(src.at[0, 0], dst.at[0, c], w_sem.at[0, i]).wait()
                got(dst.at[0, 1 - c], wp_rsem.at[0, i])
        if t == 1:
            @pl.when(p < 2)
            def _():
                for i, (src, dst) in enumerate(mats):
                    pltpu.make_async_copy(src.at[1, 0], dst.at[1, c], w_sem.at[1, i]).wait()
                    got(dst.at[1, 1 - c], wp_rsem.at[1, i])

        for h in range(H):
            if near:
                got(ag.at[t, h, 3, 0:near], (rl_rsem if h == 0 else rr_rsem).at[t % 2])
            rows = ag[t, h].astype(F32).reshape(TOK, DH).astype(BF16)
            at = pl.ds(h * DH, DH)
            for i in range(2):
                g = jnp.dot(rows, wg[sel, i, at, :], preferred_element_type=F32)
                u = jnp.dot(rows, wu[sel, i, at, :], preferred_element_type=F32)
                if h == 0:
                    acc[i] = g
                    acc[2 + i] = u
                else:
                    g = acc[i] + g
                    u = acc[2 + i] + u
                    hid[i] = (g / (1.0 + jnp.exp(-g)) * u).astype(BF16)
        if t == 0:
            pltpu.make_async_copy(dw.at[0, 0], wd.at[0, c], w_sem.at[0, 2]).wait()
            got(wd.at[0, 1 - c], wp_rsem.at[0, 2])

        for h in range(H):
            part = jnp.dot(hid[0], wd[sel, 0, :, h * DH:(h + 1) * DH], preferred_element_type=F32)
            part += jnp.dot(hid[1], wd[sel, 1, :, h * DH:(h + 1) * DH], preferred_element_type=F32)
            part = part.reshape(NX, NZ, CAP, DH)
            s1[t, h] = part[3].astype(BF16)
            pf[h] = part[0:3]
            plain[t, h] = part[1 + h].astype(BF16)
            for k in range(near, NZ):
                s2[t, h, k] = part[2 - h, k].astype(BF16)
            ahead, behind = (right, left) if h == 0 else (left, right)
            d_sem, p_sem = (d_rsem, p_rsem) if h == 0 else (e_rsem, q_rsem)
            for k in reversed(range(near, NZ)):
                send(s1.at[t, h, k], s1r.at[t, h, k], x_ssem.at[12], u_rsem.at[t % 2, h, k], across)
                send(s2.at[t, h, k], s2r.at[t, h, k], x_ssem.at[6 + h], d_sem.at[t % 2, k], ahead)
                send(plain.at[t, h, k], plainr.at[t, h, k], x_ssem.at[9 + h], p_sem.at[t % 2, k], behind)
            for k in reversed(range(near)):
                send(s1.at[t, h, k], s1r.at[t, h, k], x_ssem.at[4 + h], (a_rsem if h == 0 else c_rsem).at[t % 2, k], ahead)
        if near:
            at = slice(0, near)
            send(plain.at[t, 1, at], plainr.at[t, 1, at], x_ssem.at[10], q_rsem.at[t % 2, 0], right)
            send(plain.at[t, 0, at], plainr.at[t, 0, at], x_ssem.at[9], p_rsem.at[t % 2, 0], left)

        def middle(k):
            got(s1r.at[t, 0, k], a_rsem.at[t % 2, k])
            s2[t, 0, k] = (pf[0, 2, k] + s1r[t, 0, k].astype(F32)).astype(BF16)
            send(s2.at[t, 0, k], s2r.at[t, 0, k], x_ssem.at[6], d_rsem.at[t % 2, k], right)
            got(s1r.at[t, 1, k], c_rsem.at[t % 2, k])
            s2[t, 1, k] = (pf[1, 1, k] + s1r[t, 1, k].astype(F32)).astype(BF16)
            send(s2.at[t, 1, k], s2r.at[t, 1, k], x_ssem.at[7], e_rsem.at[t % 2, k], left)

        def final(k):
            if k >= near:
                for h in range(H):
                    got(s1r.at[t, h, k], u_rsem.at[t % 2, h, k])
                    got(plainr.at[t, h, k], (p_rsem if h == 0 else q_rsem).at[t % 2, k])
            got(s2r.at[t, 0, k], d_rsem.at[t % 2, k])
            got(s2r.at[t, 1, k], e_rsem.at[t % 2, k])
            for h in range(H):
                total = pf[h, 0, k] + s2r[t, h, k].astype(F32) + plainr[t, h, k].astype(F32)
                if k >= near:
                    total += s1r[t, h, k].astype(F32)
                eob[t, k, h] = total.astype(BF16)
            send(eob.at[t, k], ret.at[t, z], x_ssem.at[8], r_rsem.at[t], dev(home, home_z(t, k), x, other(t)))

        for k in reversed(range(near)):
            middle(k)
        for k in reversed(range(near, NZ)):
            final(k)
        if near:
            got(plainr.at[t, 0, 0:near], p_rsem.at[t % 2, 0])
            got(plainr.at[t, 1, 0:near], q_rsem.at[t % 2, 0])
        for k in reversed(range(near)):
            final(k)
        before_end()
        got(ret.at[t], r_rsem.at[t])

    def experts_sent():
        sent(ag.at[:, :, 0], x_ssem.at[0])
        sent(ag.at[:, :, 0], x_ssem.at[1])
        if near:
            sent(ag.at[:, 0, 1, 0:near], x_ssem.at[2])
            sent(ag.at[:, 1, 2, 0:near], x_ssem.at[3])
            sent(s1.at[:, 0, 0:near], x_ssem.at[4])
            sent(s1.at[:, 1, 0:near], x_ssem.at[5])
        if near < NZ:
            sent(ag.at[:, :, 3, near:], x_ssem.at[11])
            sent(s1.at[:, :, near:], x_ssem.at[12])
        sent(s2.at[:, 0], x_ssem.at[6])
        sent(s2.at[:, 1], x_ssem.at[7])
        sent(eob, x_ssem.at[8])
        sent(plain.at[:, 0], x_ssem.at[9])
        sent(plain.at[:, 1], x_ssem.at[10])

    def combine(t, xref, mix, h):
        rows = returned(t, h)
        rows = jnp.concatenate([rows, rows, jnp.zeros((64, DH), F32)], axis=0).astype(BF16)
        return xref[h].astype(F32) + jnp.dot(mix, rows, preferred_element_type=F32)

    def prepare(tab, xref):
        pick = chosen(tab)

        def one(h):
            pre[h] = jnp.dot(pick, xref[h], preferred_element_type=F32)

        each(one)

    def choose_rows(t, tab, tab_next):
        pick = chosen(tab_next)
        high, low = halves(tab)
        high = lax.dot_general(pick, high.astype(BF16), NT, preferred_element_type=F32)
        low = lax.dot_general(pick, low.astype(BF16), NT, preferred_element_type=F32)
        cross = jnp.concatenate([high, low], axis=0).astype(BF16)

        def one(h):
            added = jnp.dot(cross, returned(t, h).astype(BF16), preferred_element_type=F32)
            value = pre[h] + (added[0:SLOTS] + added[SLOTS:])
            rw[h] = value.astype(BF16).astype(F32)

        each(one)

    pltpu.make_async_copy(x0, x0, in_sem.at[0]).wait()
    pltpu.make_async_copy(gain.at[0], ga, in_sem.at[1]).wait()
    pltpu.make_async_copy(gain.at[v2], gc, in_sem.at[2]).wait()
    pick0 = chosen(mt[0])

    def gather(h):
        rw[h] = jnp.dot(pick0, x0[h], preferred_element_type=F32)

    for i, (src, dst) in enumerate(mats):
        pltpu.make_async_copy(src.at[0, 0], dst.at[0, c], w_sem.at[0, i]).start()
    each(gather)
    go = dispatch(0, ga, 0, True)
    pl.semaphore_wait(barrier, len(peers))
    for i, (src, dst) in enumerate(mats):
        send(src.at[0, 0], dst.at[0, c], wp_ssem.at[0, i], wp_rsem.at[0, i], partner)
    go()

    def background():
        send(mt.at[0], tab_a, t_ssem.at[0], t_rsem.at[0], same(2))
        send(mt.at[1], tab_b, t_ssem.at[1], t_rsem.at[1], same(1))
        send(mt.at[2], tab_c, t_ssem.at[2], t_rsem.at[2], same(1))
        send(gain.at[v1], gb, t_ssem.at[3], t_rsem.at[3], same(1))
        each(lambda h: send(x0.at[h], x1.at[h], b_ssem.at[0], b_rsem.at[0], same(2)))

        @pl.when(p < 2)
        def _():
            for i, (src, dst) in enumerate(mats):
                pltpu.make_async_copy(src.at[1, 0], dst.at[1, c], w_sem.at[1, i]).start()
                send(src.at[1, 0], dst.at[1, c], wp_ssem.at[1, i], wp_rsem.at[1, i], partner)

    def ready1():
        got(tab_a, t_rsem.at[0])
        got(tab_b, t_rsem.at[1])
        got(gb, t_rsem.at[3])
        got(x1, b_rsem.at[0])
        prepare(tab_b[...], x1)

    def nothing():
        pass

    expert(0, 0, True, 2, nothing, background, ready1)

    choose_rows(0, tab_a[...], tab_b[...])
    dispatch(1, gb, 7, False)()

    def update1():
        mix = mixer(tab_a[...])

        def one(h):
            xs[h] = combine(0, x1, mix, h).astype(BF16)

        each(one)

    expert(1, v1, False, 1, update1, nothing, lambda: prepare(mt[2], xs))

    choose_rows(1, tab_b[...], mt[2])
    dispatch(2, gc, 0, not CROSS[2])()

    def update2():
        mix = mixer(tab_b[...])

        def one(h):
            xs2[h] = combine(1, xs, mix, h).astype(BF16)
            send(xs2.at[h], x3.at[h], b_ssem.at[1], b_rsem.at[1], same(1))

        each(one)

    def ready3():
        got(tab_c, t_rsem.at[2])
        got(x3, b_rsem.at[1])

    expert(2, v2, not CROSS[2], 1, nothing, update2, ready3)
    mix_c = mixer(tab_c[...])

    def finish(h):
        out[0, :, cols(h)] = combine(2, x3, mix_c, h).astype(BF16)

    each(finish)

    for t in range(TICKS):
        n = 4 if t == 1 or CROSS[t] else 3
        sent(zs.at[t, 0:n], z_ssem.at[t])
    experts_sent()
    for i, (src, dst) in enumerate(mats):
        sent(src.at[0, 0], wp_ssem.at[0, i])
    for i in range(3):
        sent(mt.at[i], t_ssem.at[i])
    sent(gb, t_ssem.at[3])
    sent(x0, b_ssem.at[0])
    sent(xs2, b_ssem.at[1])

    @pl.when(p < 2)
    def _():
        for i, (src, dst) in enumerate(mats):
            sent(src.at[1, 0], wp_ssem.at[1, i])


def per_device(acts, routes, gates, norm_gain, gate_weight, up_weight, down_weight):
    h = lambda a: pltpu.with_memory_space_constraint(a, pltpu.HBM)
    anyw = pl.BlockSpec(memory_space=pl.ANY)
    vmem = pl.BlockSpec(memory_space=pltpu.VMEM)
    V = pltpu.VMEM
    S = pltpu.SemaphoreType.DMA
    bulk = (H, TOK, DH)
    T = (SLOTS, TOK)
    scratch = [
        V(bulk, BF16), V(bulk, BF16), V(bulk, BF16), V(bulk, BF16), V(bulk, BF16),
        V((1, D), F32), V((1, D), F32), V((1, D), F32),
        V((TICKS, SLOTS, TOK), F32), V(T, F32), V(T, F32), V(T, F32),
        V((2, 2, D, HID), BF16), V((2, 2, D, HID), BF16), V((2, 2, HID, D), BF16),
        V((TICKS, H, NX, NZ, CAP, DH), BF16),
        V((TICKS, EXPERTS, H, CAP, DH), BF16),
        V((H, SLOTS, DH), F32), V((H, SLOTS, DH), F32),
        V((4, TOK, HID), F32),
        V((2, TOK, HID), BF16),
        V((H, 3, NZ, CAP, DH), F32),
        V((TICKS, H, NZ, CAP, DH), BF16), V((TICKS, H, NZ, CAP, DH), BF16),
        V((TICKS, H, NZ, CAP, DH), BF16), V((TICKS, H, NZ, CAP, DH), BF16),
        V((TICKS, H, NZ, CAP, DH), BF16), V((TICKS, H, NZ, CAP, DH), BF16),
        V((TICKS, NZ, H, CAP, DH), BF16),
        V((TICKS, EXPERTS, H, CAP, DH), BF16),
        S((3,)), S((2, 3)), S((2, 3)), S((2, 3)), S((4,)), S((4,)), S((2,)), S((2,)),
    ]
    scratch += [S((13,)), S((TICKS,)), S((TICKS, NZ)), S((2, NZ)), S((2, NZ)), S((2,)), S((2,))]
    scratch += [S((2, NZ))] * 4 + [S((2, NZ))] * 3 + [S((2, 2, NZ)), S((TICKS,))]
    return pl.pallas_call(
        kernel,
        out_shape=jax.ShapeDtypeStruct((1, TOK, D), BF16),
        in_specs=[anyw, vmem, vmem, anyw, anyw, anyw, anyw],
        out_specs=vmem,
        scratch_shapes=scratch,
        compiler_params=pltpu.CompilerParams(
            collective_id=0, has_side_effects=True, vmem_limit_bytes=48 * 1024 * 1024
        ),
    )(h(acts), h(routes.transpose(0, 1, 3, 2)), h(gates.transpose(0, 1, 3, 2)), h(norm_gain), h(gate_weight), h(up_weight), h(down_weight))


def solution(mesh):
    return jax.shard_map(
        per_device,
        mesh=mesh,
        in_specs=(
            P("pipe", "expert", None),
            P(None, "pipe", "expert", None),
            P(None, "pipe", "expert", None),
            P(None, "pipe", None),
            P(None, "pipe", None, "expert"),
            P(None, "pipe", None, "expert"),
            P(None, "pipe", "expert", None),
        ),
        out_specs=P("pipe", "expert", None),
        check_vma=False,
    )
```

```python
import jax
import jax.numpy as jnp
from jax import lax
from jax.experimental import pallas as pl
from jax.experimental.pallas import tpu as pltpu
from jax.sharding import PartitionSpec as P

CAP = 8
TOPK = 8
EXPERTS = 4
NP = 8
NZ = 4
NX = 4
D = 3584
H = 2
DH = D // H
TOK = 128
HID = 256
TICKS = 3
DORD = (0, 1, 2, 3)
CROSS = (0, 0, 0)
EARLY = 2
LATE = 2
GATHER_NEAR = (3, 2, 3)
MID = 1
SLOTS = EXPERTS * CAP
epsilon = 1e-06
F32 = jnp.float32
BF16 = jnp.bfloat16
MESH = pl.DeviceIdType.MESH
NT = (((1,), (1,)), ((), ()))


def kernel(
    acts, routes_hbm, gates_hbm, gain, gw, uw, dw, out,
    routes, gates,    x0, x1, xs, xs2, x3, ga, gb, gc, mt, tab_a, tab_b, tab_c, mix_c,
    wg, wu, wd, ag, zs, rw, pre, acc, hid, pf, s1, s1r, s2, s2r, plain, plainr, eob, ret,
    in_sem, w_sem, wp_ssem, wp_rsem, t_ssem, t_rsem, b_ssem, b_rsem,
    x_ssem, z_ssem, z_rsem, y_rsem, xl_rsem, xr_rsem, rl_rsem, rr_rsem, a_rsem, c_rsem, d_rsem, e_rsem, p_rsem, q_rsem, v_rsem, u_rsem, r_rsem,
):
    p = lax.axis_index("pipe")
    q = lax.axis_index("expert")
    z = q // 8
    x = lax.rem(q // 2, NX)
    c = lax.rem(q, 2)
    odd = lax.rem(p, 2)

    def dev(dp, zz, xx, cc):
        return {"pipe": lax.rem(p + dp, NP), "expert": zz * 8 + xx * 2 + cc}

    def same(dp):
        return dev(dp, z, x, c)

    def other(t):
        return 1 - c if CROSS[t] else c

    near = NZ - 1
    partner = dev(0, z, x, 1 - c)
    right = dev(0, z, lax.rem(x + 1, NX), c)
    left = dev(0, z, lax.rem(x + 3, NX), c)
    across = dev(0, z, lax.rem(x + 2, NX), c)

    def rc(src, dst, ss, rs, to):
        return pltpu.make_async_remote_copy(
            src_ref=src, dst_ref=dst, send_sem=ss, recv_sem=rs, device_id=to, device_id_type=MESH
        )

    def send(src, dst, ss, rs, to):
        rc(src, dst, ss, rs, to).start()

    def got(ref, sem):
        rc(ref, ref, sem, sem, right).wait_recv()

    def sent(ref, sem):
        rc(ref, ref, sem, sem, right).wait_send()

    def each(body):
        lax.fori_loop(0, H, lambda h, carry: (body(h), carry)[1], 0)

    def cols(h):
        return pl.ds(pl.multiple_of(h * DH, 128), DH)

    def z_even(offset):
        return lax.rem(z + offset, NZ)

    def z_next(k):
        if k == 0 or k == 3:
            return lax.rem(z + (0, 0, 0, 2)[k], NZ)
        return lax.rem(z + (2 * odd + 3 if k == 1 else 5 - 2 * odd), NZ)

    def dst_z(t, k):
        return z_next(k) if t == 1 else z_even((0, 1, 3, 2)[k])

    def home_z(t, k):
        return z_next(k) if t == 1 else z_even((0, 3, 1, 2)[k])

    loads = [(routes_hbm, routes), (gates_hbm, gates), (gain.at[0], ga), (gain.at[(9 - p) // 8], gc)]
    for i, (src, dst) in enumerate(loads[:2]):
        pltpu.make_async_copy(src, dst, in_sem.at[i]).start()
    each(lambda h: pltpu.make_async_copy(acts.at[0, :, cols(h)], x0.at[h], in_sem.at[4]).start())
    for i, (src, dst) in enumerate(loads[2:]):
        pltpu.make_async_copy(src, dst, in_sem.at[2 + i]).start()

    barrier = pltpu.get_barrier_semaphore()
    flows = {(dp, cross) for t, pair in enumerate(((0, 2), (7, 1), (0, 1))) for dp in pair for cross in (CROSS[t],)}
    flows |= {((NP - dp) % NP, cross) for dp, cross in flows}
    places = {(dp, dz, cross) for dp, cross in flows for dz in range(NZ)} | {(dp, 0, 0) for dp in (1, 2, 6, 7)}
    places = sorted(places - {(0, 0, 0)} | {(0, 0, 1)})
    peers = [right, left, across] + [dev(dp, lax.rem(z + dz, NZ), x, 1 - c if cross else c) for dp, dz, cross in places]
    for peer in peers:
        pl.semaphore_signal(barrier, inc=1, device_id=peer, device_id_type=MESH)

    v1 = (8 - p) // 8
    v2 = (9 - p) // 8

    mats = ((gw, wg), (uw, wu), (dw, wd))

    earlier = (
        lax.broadcasted_iota(jnp.int32, (TOK, TOK), 0) < lax.broadcasted_iota(jnp.int32, (TOK, TOK), 1)
    ).astype(F32).astype(BF16)
    slot = lax.broadcasted_iota(jnp.int32, (CAP, TOK), 0).astype(F32)

    def table(t, carry):
        ids, values = routes[t, 0], gates[t, 0]
        taken, weight = [], []
        for e in range(EXPERTS):
            match = ids == e
            taken.append(jnp.sum(jnp.where(match, F32(1.0), F32(0.0)), axis=0, keepdims=True))
            weight.append(jnp.sum(jnp.where(match, values, F32(0.0)), axis=0, keepdims=True))
        four = jnp.concatenate(taken + [jnp.zeros((4, TOK), F32)], axis=0)
        before = jnp.dot(four.astype(BF16), earlier, preferred_element_type=F32)
        for e in range(EXPERTS):
            here = (before[e:e + 1] == slot) & (taken[e] > 0.5)
            mt[t, e * CAP:(e + 1) * CAP] = jnp.where(here, weight[e], F32(0.0))
        return carry

    for i, (src, dst) in enumerate(loads[:2]):
        pltpu.make_async_copy(src, dst, in_sem.at[i]).wait()
    lax.fori_loop(0, TICKS, table, 0)

    def chosen(tab):
        return (tab > 0).astype(F32).astype(BF16)

    def halves(tab):
        high = tab.astype(BF16).astype(F32)
        return high, tab - high

    def mixer(tab):
        high, low = halves(tab)
        return jnp.concatenate([high, low, jnp.zeros((64, TOK), F32)], axis=0).T.astype(BF16)

    def returned(t, h):
        return ret[t, :, h].astype(F32).reshape(SLOTS, DH)

    def dispatch(t, gref, dp, local):
        total = jnp.zeros((SLOTS, 1), F32)
        for h in range(H):
            total += jnp.sum(rw[h] * rw[h], axis=-1, keepdims=True)
        inverse = lax.rsqrt(total / D + epsilon)

        def scale(h):
            rows = (rw[h] * inverse * gref[:, cols(h)]).reshape(EXPERTS, CAP, DH).astype(BF16)
            zs[t, :, h] = rows

        each(scale)

        def go():
            for k in DORD:
                if not (local and k == 0):
                    zz = dst_z(t, k)
                    to = dev(dp, zz, x, other(t))
                    if k < GATHER_NEAR[t]:
                        send(zs.at[t, zz], ag.at[t, :, 0, k], z_ssem.at[t], z_rsem.at[t, k], to)
                    else:
                        for h in range(H):
                            send(zs.at[t, zz, h], ag.at[t, h, 0, k], z_ssem.at[t], y_rsem.at[t, k - 2, h], to)
            if local:
                for h in range(H):
                    ag[t, h, 0, 0] = zs[t, z, h]
        return go

    def expert(t, sel, local, home, before_first, after_first, after_z, before_end):
        def first(k):
            if k >= GATHER_NEAR[t]:
                for h in range(H):
                    got(ag.at[t, h, 0, k], y_rsem.at[t, k - 2, h])
                    v_sem = v_rsem.at[t % 2, k - 2]
                    send(ag.at[t, h, 0, k], ag.at[t, h, 3, k], x_ssem.at[11 if k == 3 else 13], v_sem.at[0, h], across)
                    send(ag.at[t, h, 0, k], ag.at[t, h, 1, k], x_ssem.at[0], v_sem.at[1, h], right)
                    send(ag.at[t, h, 0, k], ag.at[t, h, 2, k], x_ssem.at[1], v_sem.at[2, h], left)
                return
            if not (local and k == 0):
                got(ag.at[t, :, 0, k], z_rsem.at[t, k])
            send(ag.at[t, :, 0, k], ag.at[t, :, 1, k], x_ssem.at[0], xl_rsem.at[t % 2, k], right)
            send(ag.at[t, :, 0, k], ag.at[t, :, 2, k], x_ssem.at[1], xr_rsem.at[t % 2, k], left)

        def relay(k):
            got(ag.at[t, :, 1, k], xl_rsem.at[t % 2, k])
            send(ag.at[t, 0, 1, k], ag.at[t, 0, 3, k], x_ssem.at[2 if k < 2 else 14], rl_rsem.at[t % 2], right)
            got(ag.at[t, :, 2, k], xr_rsem.at[t % 2, k])
            send(ag.at[t, 1, 2, k], ag.at[t, 1, 3, k], x_ssem.at[3 if k < 2 else 15], rr_rsem.at[t % 2], left)

        before_first()
        first(0)
        after_first()
        first(1)
        first(2)
        if t == 1:
            first(3)
            relay(0)
        else:
            relay(0)
            first(3)
        after_z()
        relay(1)
        if GATHER_NEAR[t] > 2:
            relay(2)

        if t == 0:
            for i, (src, dst) in enumerate(mats[:2]):
                pltpu.make_async_copy(src.at[0, 0], dst.at[0, c], w_sem.at[0, i]).wait()
                got(dst.at[0, 1 - c], wp_rsem.at[0, i])
        if t == 1:
            @pl.when(p < 2)
            def _():
                for i, (src, dst) in enumerate(mats):
                    pltpu.make_async_copy(src.at[1, 0], dst.at[1, c], w_sem.at[1, i]).wait()
                    got(dst.at[1, 1 - c], wp_rsem.at[1, i])

        for h in range(H):
            got(ag.at[t, h, 3, 0:GATHER_NEAR[t]], (rl_rsem if h == 0 else rr_rsem).at[t % 2])
            for k in range(GATHER_NEAR[t], NZ):
                for i, slot in enumerate((3, 1, 2)):
                    got(ag.at[t, h, slot, k], v_rsem.at[t % 2, k - 2, i, h])
            rows = ag[t, h].astype(F32).reshape(TOK, DH).astype(BF16)
            at = pl.ds(h * DH, DH)
            for i in range(2):
                g = jnp.dot(rows, wg[sel, i, at, :], preferred_element_type=F32)
                u = jnp.dot(rows, wu[sel, i, at, :], preferred_element_type=F32)
                if h == 0:
                    acc[i] = g
                    acc[2 + i] = u
                else:
                    g = acc[i] + g
                    u = acc[2 + i] + u
                    hid[i] = (g / (1.0 + jnp.exp(-g)) * u).astype(BF16)
        if t == 0:
            pltpu.make_async_copy(dw.at[0, 0], wd.at[0, c], w_sem.at[0, 2]).wait()
            got(wd.at[0, 1 - c], wp_rsem.at[0, 2])

        for h in range(H):
            part = jnp.dot(hid[0], wd[sel, 0, :, h * DH:(h + 1) * DH], preferred_element_type=F32)
            part += jnp.dot(hid[1], wd[sel, 1, :, h * DH:(h + 1) * DH], preferred_element_type=F32)
            part = part.reshape(NX, NZ, CAP, DH)
            s1[t, h] = part[3].astype(BF16)
            pf[h] = part[0:3]
            plain[t, h] = part[1 + h].astype(BF16)
            for k in range(near, NZ):
                s2[t, h, k] = part[2 - h, k].astype(BF16)
            ahead, behind = (right, left) if h == 0 else (left, right)
            d_sem, p_sem = (d_rsem, p_rsem) if h == 0 else (e_rsem, q_rsem)
            a_sem = a_rsem if h == 0 else c_rsem

            def shared(k):
                send(s1.at[t, h, k], s1r.at[t, h, k], x_ssem.at[4 + h], a_sem.at[t % 2, k], ahead)

            for k in reversed(range(near - EARLY, near)):
                shared(k)
            for k in reversed(range(near, NZ)):
                send(s1.at[t, h, k], s1r.at[t, h, k], x_ssem.at[12], u_rsem.at[t % 2, h, k - near], across)
                send(s2.at[t, h, k], s2r.at[t, h, k], x_ssem.at[6 + h], d_sem.at[t % 2, k], ahead)
                send(plain.at[t, h, k], plainr.at[t, h, k], x_ssem.at[9 + h], p_sem.at[t % 2, 1 + k - near], behind)
            for k in reversed(range(near - EARLY)):
                shared(k)
        if near:
            at = slice(0, near)
            send(plain.at[t, 1, at], plainr.at[t, 1, at], x_ssem.at[10], q_rsem.at[t % 2, 0], right)
            send(plain.at[t, 0, at], plainr.at[t, 0, at], x_ssem.at[9], p_rsem.at[t % 2, 0], left)

        def middle(k):
            got(s1r.at[t, 0, k], a_rsem.at[t % 2, k])
            s2[t, 0, k] = (pf[0, 2, k] + s1r[t, 0, k].astype(F32)).astype(BF16)
            send(s2.at[t, 0, k], s2r.at[t, 0, k], x_ssem.at[6], d_rsem.at[t % 2, k], right)
            got(s1r.at[t, 1, k], c_rsem.at[t % 2, k])
            s2[t, 1, k] = (pf[1, 1, k] + s1r[t, 1, k].astype(F32)).astype(BF16)
            send(s2.at[t, 1, k], s2r.at[t, 1, k], x_ssem.at[7], e_rsem.at[t % 2, k], left)

        def final(k):
            to = dev(home, home_z(t, k), x, other(t))
            if k < near:
                got(s2r.at[t, 0, k], d_rsem.at[t % 2, k])
                got(s2r.at[t, 1, k], e_rsem.at[t % 2, k])
            for h in range(H):
                if k >= near:
                    got(s1r.at[t, h, k], u_rsem.at[t % 2, h, k - near])
                    got(plainr.at[t, h, k], (p_rsem if h == 0 else q_rsem).at[t % 2, 1 + k - near])
                    got(s2r.at[t, h, k], (d_rsem if h == 0 else e_rsem).at[t % 2, k])
                total = pf[h, 0, k] + s2r[t, h, k].astype(F32) + plainr[t, h, k].astype(F32)
                if k >= near:
                    total += s1r[t, h, k].astype(F32)
                eob[t, k, h] = total.astype(BF16)
                if k >= near:
                    send(eob.at[t, k, h], ret.at[t, z, h], x_ssem.at[8], r_rsem.at[t], to)
            if k < near:
                send(eob.at[t, k], ret.at[t, z], x_ssem.at[8], r_rsem.at[t], to)

        for k in reversed(range(MID, near)):
            middle(k)
        for k in reversed(range(near, NZ)):
            final(k)
        for k in reversed(range(MID)):
            middle(k)
        if near:
            got(plainr.at[t, 0, 0:near], p_rsem.at[t % 2, 0])
            got(plainr.at[t, 1, 0:near], q_rsem.at[t % 2, 0])
        for k in reversed(range(near)):
            final(k)
        before_end()
        got(ret.at[t], r_rsem.at[t])

    def experts_sent():
        sent(ag.at[:, :, 0], x_ssem.at[0])
        sent(ag.at[:, :, 0], x_ssem.at[1])
        sent(ag.at[:, 0, 1, 0:2], x_ssem.at[2])
        sent(ag.at[:, 1, 2, 0:2], x_ssem.at[3])
        sent(ag.at[0, :, 3, 2], x_ssem.at[13])
        sent(ag.at[0:2, 0, 1, 2], x_ssem.at[14])
        sent(ag.at[0:2, 1, 2, 2], x_ssem.at[15])
        sent(s1.at[:, 0, 0:near], x_ssem.at[4])
        sent(s1.at[:, 1, 0:near], x_ssem.at[5])
        sent(ag.at[:, :, 3, near:], x_ssem.at[11])
        sent(s1.at[:, :, near:], x_ssem.at[12])
        sent(s2.at[:, 0], x_ssem.at[6])
        sent(s2.at[:, 1], x_ssem.at[7])
        sent(plain.at[:, 0], x_ssem.at[9])
        sent(plain.at[:, 1], x_ssem.at[10])

    def combine(t, xref, mix, h):
        rows = returned(t, h)
        rows = jnp.concatenate([rows, rows, jnp.zeros((64, DH), F32)], axis=0).astype(BF16)
        return xref[h].astype(F32) + jnp.dot(mix, rows, preferred_element_type=F32)

    def prepare(tab, xref):
        pick = chosen(tab)

        def one(h):
            pre[h] = jnp.dot(pick, xref[h], preferred_element_type=F32)

        each(one)

    def choose_rows(t, tab, tab_next):
        pick = chosen(tab_next)
        high, low = halves(tab)
        high = lax.dot_general(pick, high.astype(BF16), NT, preferred_element_type=F32)
        low = lax.dot_general(pick, low.astype(BF16), NT, preferred_element_type=F32)
        cross = jnp.concatenate([high, low], axis=0).astype(BF16)

        def one(h):
            added = jnp.dot(cross, returned(t, h).astype(BF16), preferred_element_type=F32)
            value = pre[h] + (added[0:SLOTS] + added[SLOTS:])
            rw[h] = value.astype(BF16).astype(F32)

        each(one)

    pltpu.make_async_copy(x0, x0, in_sem.at[4]).wait()
    for i, (src, dst) in enumerate(loads[2:]):
        pltpu.make_async_copy(src, dst, in_sem.at[2 + i]).wait()
    pick0 = chosen(mt[0])

    def gather(h):
        rw[h] = jnp.dot(pick0, x0[h], preferred_element_type=F32)

    for i, (src, dst) in enumerate(mats):
        pltpu.make_async_copy(src.at[0, 0], dst.at[0, c], w_sem.at[0, i]).start()
    each(gather)
    go = dispatch(0, ga, 0, True)
    pl.semaphore_wait(barrier, len(peers))
    for i, (src, dst) in enumerate(mats):
        send(src.at[0, 0], dst.at[0, c], wp_ssem.at[i], wp_rsem.at[0, i], partner)
    go()

    def background():
        send(mt.at[0], tab_a, t_ssem.at[0], t_rsem.at[0], same(2))
        send(mt.at[1], tab_b, t_ssem.at[1], t_rsem.at[1], same(1))
        send(mt.at[2], tab_c, t_ssem.at[2], t_rsem.at[2], same(1))
        send(gain.at[v1], gb, t_ssem.at[3], t_rsem.at[3], same(1))
        each(lambda h: send(x0.at[h], x1.at[h], b_ssem.at[0], b_rsem.at[0], same(2)))

        @pl.when(p < 2)
        def _():
            for i, (src, dst) in enumerate(mats):
                pltpu.make_async_copy(src.at[1, 0], dst.at[1, c], w_sem.at[1, i]).start()
                send(src.at[1, 0], dst.at[1, c], wp_ssem.at[3 + i], wp_rsem.at[1, i], partner)

    def ready1():
        got(tab_a, t_rsem.at[0])
        got(tab_b, t_rsem.at[1])
        got(gb, t_rsem.at[3])
        got(x1, b_rsem.at[0])
        prepare(tab_b[...], x1)

    def nothing():
        pass

    expert(0, 0, True, 2, nothing, background, nothing, ready1)

    choose_rows(0, tab_a[...], tab_b[...])
    dispatch(1, gb, 7, False)()

    def update1():
        mix = mixer(tab_a[...])

        def one(h):
            xs[h] = combine(0, x1, mix, h).astype(BF16)

        each(one)

    expert(1, v1, False, 1, update1, nothing, nothing, lambda: prepare(mt[2], xs))

    choose_rows(1, tab_b[...], mt[2])
    dispatch(2, gc, 0, not CROSS[2])()

    def update2():
        mix = mixer(tab_b[...])

        def one(h):
            xs2[h] = combine(1, xs, mix, h).astype(BF16)

        each(one)
        for h in range(LATE):
            send(xs2.at[h], x3.at[h], b_ssem.at[1], b_rsem.at[1], same(1))

    def ahead2():
        for h in range(LATE, H):
            send(xs2.at[h], x3.at[h], b_ssem.at[1], b_rsem.at[1], same(1))

    def ready3():
        got(tab_c, t_rsem.at[2])
        mix_c[...] = mixer(tab_c[...])
        got(x3, b_rsem.at[1])
        for t in range(TICKS):
            n = 4 if t == 1 or CROSS[t] else 3
            sent(zs.at[t, 0:n], z_ssem.at[t])
        experts_sent()
        for i, (src, dst) in enumerate(mats):
            sent(src.at[0, 0], wp_ssem.at[i])
        for i in range(3):
            sent(mt.at[i], t_ssem.at[i])
        sent(gb, t_ssem.at[3])
        sent(x0, b_ssem.at[0])
        sent(xs2, b_ssem.at[1])

        @pl.when(p < 2)
        def _():
            for i, (src, dst) in enumerate(mats):
                sent(src.at[1, 0], wp_ssem.at[3 + i])

    expert(2, v2, not CROSS[2], 1, nothing, update2, ahead2, ready3)
    def finish(h):
        out[0, :, cols(h)] = combine(2, x3, mix_c[...], h).astype(BF16)

    each(finish)
    sent(eob, x_ssem.at[8])


def per_device(acts, routes, gates, norm_gain, gate_weight, up_weight, down_weight):
    h = lambda a: pltpu.with_memory_space_constraint(a, pltpu.HBM)
    anyw = pl.BlockSpec(memory_space=pl.ANY)
    vmem = pl.BlockSpec(memory_space=pltpu.VMEM)
    V = pltpu.VMEM
    S = pltpu.SemaphoreType.DMA
    bulk = (H, TOK, DH)
    T = (SLOTS, TOK)
    scratch = [
        V((TICKS, 1, TOPK, TOK), jnp.int32), V((TICKS, 1, TOPK, TOK), F32),
        V(bulk, BF16), V(bulk, BF16), V(bulk, BF16), V(bulk, BF16), V(bulk, BF16),
        V((1, D), F32), V((1, D), F32), V((1, D), F32),
        V((TICKS, SLOTS, TOK), F32), V(T, F32), V(T, F32), V(T, F32), V((TOK, TOK), BF16),
        V((2, 2, D, HID), BF16), V((2, 2, D, HID), BF16), V((2, 2, HID, D), BF16),
        V((TICKS, H, NX, NZ, CAP, DH), BF16),
        V((TICKS, EXPERTS, H, CAP, DH), BF16),
        V((H, SLOTS, DH), F32), V((H, SLOTS, DH), F32),
        V((4, TOK, HID), F32),
        V((2, TOK, HID), BF16),
        V((H, 3, NZ, CAP, DH), F32),
        V((TICKS, H, NZ, CAP, DH), BF16), V((TICKS, H, NZ, CAP, DH), BF16),
        V((TICKS, H, NZ, CAP, DH), BF16), V((TICKS, H, NZ, CAP, DH), BF16),
        V((TICKS, H, NZ, CAP, DH), BF16), V((TICKS, H, NZ, CAP, DH), BF16),
        V((TICKS, NZ, H, CAP, DH), BF16),
        V((TICKS, EXPERTS, H, CAP, DH), BF16),
        S((5,)), S((2, 3)), S((6,)), S((2, 3)), S((4,)), S((4,)), S((2,)), S((2,)),
    ]
    scratch += [S((16,)), S((TICKS,)), S((TICKS, 3)), S((TICKS, 2, H)), S((2, 3)), S((2, 3)), S((2,)), S((2,))]
    scratch += [S((2, 3))] * 2 + [S((2, NZ))] * 2 + [S((2, 2))] * 2 + [S((2, 2, 3, H)), S((2, H, 1)), S((TICKS,))]
    return pl.pallas_call(
        kernel,
        out_shape=jax.ShapeDtypeStruct((1, TOK, D), BF16),
        in_specs=[anyw, anyw, anyw, anyw, anyw, anyw, anyw],
        out_specs=vmem,
        scratch_shapes=scratch,
        compiler_params=pltpu.CompilerParams(
            collective_id=0, has_side_effects=True, vmem_limit_bytes=48 * 1024 * 1024
        ),
    )(h(acts), h(routes.transpose(0, 1, 3, 2)), h(gates.transpose(0, 1, 3, 2)), h(norm_gain), h(gate_weight), h(up_weight), h(down_weight))


def solution(mesh):
    return jax.shard_map(
        per_device,
        mesh=mesh,
        in_specs=(
            P("pipe", "expert", None),
            P(None, "pipe", "expert", None),
            P(None, "pipe", "expert", None),
            P(None, "pipe", None),
            P(None, "pipe", None, "expert"),
            P(None, "pipe", None, "expert"),
            P(None, "pipe", "expert", None),
        ),
        out_specs=P("pipe", "expert", None),
        check_vma=False,
    )
```

```python
import jax
import jax.numpy as jnp
from jax import lax
from jax.experimental import pallas as pl
from jax.experimental.pallas import tpu as pltpu
from jax.sharding import PartitionSpec as P

CAP = 8
TOPK = 8
EXPERTS = 4
NP = 8
NZ = 4
NX = 4
D = 3584
H = 2
DH = D // H
TOK = 128
HID = 256
TICKS = 3
DORD = (0, 1, 2, 3)
CROSS = (0, 0, 0)
EARLY = 2
LATE = 2
GATHER_NEAR = (3, 2, 3)
MID = 1
SLOTS = EXPERTS * CAP
epsilon = 1e-06
F32 = jnp.float32
BF16 = jnp.bfloat16
MESH = pl.DeviceIdType.MESH
NT = (((1,), (1,)), ((), ()))


def kernel(
    acts, routes_hbm, gates_hbm, gain, gw, uw, dw, out,
    routes, gates,    x0, x1, xs, xs2, x3, ga, gb, gc, mt, tab_a, tab_b, tab_c, mix_c,
    wg, wu, wd, ag, zs, rw, pre, acc, hid, pf, s1, s1r, s2, s2r, plain, plainr, eob, ret,
    in_sem, w_sem, wp_ssem, wp_rsem, t_ssem, t_rsem, b_ssem, b_rsem,
    x_ssem, z_ssem, z_rsem, y_rsem, xl_rsem, xr_rsem, rl_rsem, rr_rsem, a_rsem, c_rsem, d_rsem, e_rsem, p_rsem, q_rsem, v_rsem, u_rsem, r_rsem,
):
    p = lax.axis_index("pipe")
    q = lax.axis_index("expert")
    z = q // 8
    x = lax.rem(q // 2, NX)
    c = lax.rem(q, 2)
    odd = lax.rem(p, 2)

    def dev(dp, zz, xx, cc):
        return {"pipe": lax.rem(p + dp, NP), "expert": zz * 8 + xx * 2 + cc}

    def same(dp):
        return dev(dp, z, x, c)

    def other(t):
        return 1 - c if CROSS[t] else c

    near = NZ - 1
    partner = dev(0, z, x, 1 - c)
    right = dev(0, z, lax.rem(x + 1, NX), c)
    left = dev(0, z, lax.rem(x + 3, NX), c)
    across = dev(0, z, lax.rem(x + 2, NX), c)

    def rc(src, dst, ss, rs, to):
        return pltpu.make_async_remote_copy(
            src_ref=src, dst_ref=dst, send_sem=ss, recv_sem=rs, device_id=to, device_id_type=MESH
        )

    def send(src, dst, ss, rs, to):
        rc(src, dst, ss, rs, to).start()

    def got(ref, sem):
        rc(ref, ref, sem, sem, right).wait_recv()

    def sent(ref, sem):
        rc(ref, ref, sem, sem, right).wait_send()

    def each(body):
        lax.fori_loop(0, H, lambda h, carry: (body(h), carry)[1], 0)

    def cols(h):
        return pl.ds(pl.multiple_of(h * DH, 128), DH)

    def z_even(offset):
        return lax.rem(z + offset, NZ)

    def z_next(k):
        if k == 0 or k == 3:
            return lax.rem(z + (0, 0, 0, 2)[k], NZ)
        return lax.rem(z + (2 * odd + 3 if k == 1 else 5 - 2 * odd), NZ)

    def dst_z(t, k):
        return z_next(k) if t == 1 else z_even((0, 1, 3, 2)[k])

    def home_z(t, k):
        return z_next(k) if t == 1 else z_even((0, 3, 1, 2)[k])

    loads = [(routes_hbm, routes), (gates_hbm, gates), (gain.at[0], ga), (gain.at[(9 - p) // 8], gc)]
    for i, (src, dst) in enumerate(loads[:2]):
        pltpu.make_async_copy(src, dst, in_sem.at[i]).start()
    each(lambda h: pltpu.make_async_copy(acts.at[0, :, cols(h)], x0.at[h], in_sem.at[4]).start())
    for i, (src, dst) in enumerate(loads[2:]):
        pltpu.make_async_copy(src, dst, in_sem.at[2 + i]).start()

    barrier = pltpu.get_barrier_semaphore()
    flows = {(dp, cross) for t, pair in enumerate(((0, 2), (7, 1), (0, 1))) for dp in pair for cross in (CROSS[t],)}
    flows |= {((NP - dp) % NP, cross) for dp, cross in flows}
    places = {(dp, dz, cross) for dp, cross in flows for dz in range(NZ)} | {(dp, 0, 0) for dp in (1, 2, 6, 7)}
    places = sorted(places - {(0, 0, 0)} | {(0, 0, 1)})
    peers = [right, left, across] + [dev(dp, lax.rem(z + dz, NZ), x, 1 - c if cross else c) for dp, dz, cross in places]
    for peer in peers:
        pl.semaphore_signal(barrier, inc=1, device_id=peer, device_id_type=MESH)

    v1 = (8 - p) // 8
    v2 = (9 - p) // 8

    mats = ((gw, wg), (uw, wu), (dw, wd))

    earlier = (
        lax.broadcasted_iota(jnp.int32, (TOK, TOK), 0) < lax.broadcasted_iota(jnp.int32, (TOK, TOK), 1)
    ).astype(F32).astype(BF16)
    slot = lax.broadcasted_iota(jnp.int32, (CAP, TOK), 0).astype(F32)

    def table(t, carry):
        ids, values = routes[t, 0], gates[t, 0]
        taken, weight = [], []
        for e in range(EXPERTS):
            match = ids == e
            taken.append(jnp.sum(jnp.where(match, F32(1.0), F32(0.0)), axis=0, keepdims=True))
            weight.append(jnp.sum(jnp.where(match, values, F32(0.0)), axis=0, keepdims=True))
        four = jnp.concatenate(taken + [jnp.zeros((4, TOK), F32)], axis=0)
        before = jnp.dot(four.astype(BF16), earlier, preferred_element_type=F32)
        for e in range(EXPERTS):
            here = (before[e:e + 1] == slot) & (taken[e] > 0.5)
            mt[t, e * CAP:(e + 1) * CAP] = jnp.where(here, weight[e], F32(0.0))
        return carry

    for i, (src, dst) in enumerate(loads[:2]):
        pltpu.make_async_copy(src, dst, in_sem.at[i]).wait()
    lax.fori_loop(0, TICKS, table, 0)

    def chosen(tab):
        return (tab > 0).astype(F32).astype(BF16)

    def halves(tab):
        high = tab.astype(BF16).astype(F32)
        return high, tab - high

    def mixer(tab):
        high, low = halves(tab)
        return jnp.concatenate([high, low], axis=0).T.astype(BF16)

    def returned(t, h):
        return ret[t, :, h].astype(F32).reshape(SLOTS, DH)

    def dispatch(t, gref, dp, local):
        total = jnp.zeros((SLOTS, 1), F32)
        for h in range(H):
            total += jnp.sum(rw[h] * rw[h], axis=-1, keepdims=True)
        inverse = lax.rsqrt(total / D + epsilon)

        def scale(h):
            rows = (rw[h] * inverse * gref[:, cols(h)]).reshape(EXPERTS, CAP, DH).astype(BF16)
            zs[t, :, h] = rows

        each(scale)

        def go():
            for k in DORD:
                if not (local and k == 0):
                    zz = dst_z(t, k)
                    to = dev(dp, zz, x, other(t))
                    if k < GATHER_NEAR[t]:
                        send(zs.at[t, zz], ag.at[t, :, 0, k], z_ssem.at[t], z_rsem.at[t, k], to)
                    else:
                        for h in range(H):
                            send(zs.at[t, zz, h], ag.at[t, h, 0, k], z_ssem.at[t], y_rsem.at[t, k - 2, h], to)
            if local:
                for h in range(H):
                    ag[t, h, 0, 0] = zs[t, z, h]
        return go

    def expert(t, sel, local, home, before_first, after_first, after_z, before_end):
        def first(k):
            if k >= GATHER_NEAR[t]:
                for h in range(H):
                    got(ag.at[t, h, 0, k], y_rsem.at[t, k - 2, h])
                    v_sem = v_rsem.at[t % 2, k - 2, h]
                    send(ag.at[t, h, 0, k], ag.at[t, h, 3, k], x_ssem.at[11 if k == 3 else 13], v_sem, across)
                    send(ag.at[t, h, 0, k], ag.at[t, h, 1, k], x_ssem.at[0], v_sem, right)
                    send(ag.at[t, h, 0, k], ag.at[t, h, 2, k], x_ssem.at[1], v_sem, left)
                return
            if not (local and k == 0):
                got(ag.at[t, :, 0, k], z_rsem.at[t, k])
            send(ag.at[t, :, 0, k], ag.at[t, :, 1, k], x_ssem.at[0], xl_rsem.at[t % 2, k], right)
            send(ag.at[t, :, 0, k], ag.at[t, :, 2, k], x_ssem.at[1], xr_rsem.at[t % 2, k], left)

        def relay(k):
            got(ag.at[t, :, 1, k], xl_rsem.at[t % 2, k])
            send(ag.at[t, 0, 1, k], ag.at[t, 0, 3, k], x_ssem.at[2 if k < 2 else 14], rl_rsem.at[t % 2], right)
            got(ag.at[t, :, 2, k], xr_rsem.at[t % 2, k])
            send(ag.at[t, 1, 2, k], ag.at[t, 1, 3, k], x_ssem.at[3 if k < 2 else 15], rr_rsem.at[t % 2], left)

        before_first()
        first(0)
        after_first()
        first(1)
        first(2)
        if t == 1:
            first(3)
            relay(0)
        else:
            relay(0)
            first(3)
        after_z()
        relay(1)
        if GATHER_NEAR[t] > 2:
            relay(2)

        if t == 0:
            for i, (src, dst) in enumerate(mats[:2]):
                pltpu.make_async_copy(src.at[0, 0], dst.at[0, c], w_sem.at[0, i]).wait()
                got(dst.at[0, 1 - c], wp_rsem.at[0, i])
        if t == 1:
            @pl.when(p < 2)
            def _():
                for i, (src, dst) in enumerate(mats):
                    pltpu.make_async_copy(src.at[1, 0], dst.at[1, c], w_sem.at[1, i]).wait()
                    got(dst.at[1, 1 - c], wp_rsem.at[1, i])

        for h in range(H):
            got(ag.at[t, h, 3, 0:GATHER_NEAR[t]], (rl_rsem if h == 0 else rr_rsem).at[t % 2])
            for k in range(GATHER_NEAR[t], NZ):
                got(ag.at[t, h, 1:NX, k], v_rsem.at[t % 2, k - 2, h])
            rows = ag[t, h].astype(F32).reshape(TOK, DH).astype(BF16)
            at = pl.ds(h * DH, DH)
            for i in range(2):
                g = jnp.dot(rows, wg[sel, i, at, :], preferred_element_type=F32)
                u = jnp.dot(rows, wu[sel, i, at, :], preferred_element_type=F32)
                if h == 0:
                    acc[i] = g
                    acc[2 + i] = u
                else:
                    g = acc[i] + g
                    u = acc[2 + i] + u
                    hid[i] = (g / (1.0 + jnp.exp(-g)) * u).astype(BF16)
        if t == 0:
            pltpu.make_async_copy(dw.at[0, 0], wd.at[0, c], w_sem.at[0, 2]).wait()
            got(wd.at[0, 1 - c], wp_rsem.at[0, 2])

        for h in range(H):
            part = jnp.dot(hid[0], wd[sel, 0, :, h * DH:(h + 1) * DH], preferred_element_type=F32)
            part += jnp.dot(hid[1], wd[sel, 1, :, h * DH:(h + 1) * DH], preferred_element_type=F32)
            part = part.reshape(NX, NZ, CAP, DH)
            s1[t, h] = part[3].astype(BF16)
            pf[h] = part[0:3]
            plain[t, h] = part[1 + h].astype(BF16)
            for k in range(near, NZ):
                s2[t, h, k] = part[2 - h, k].astype(BF16)
            ahead, behind = (right, left) if h == 0 else (left, right)
            d_sem, p_sem = (d_rsem, p_rsem) if h == 0 else (e_rsem, q_rsem)
            a_sem = a_rsem if h == 0 else c_rsem

            def shared(k):
                send(s1.at[t, h, k], s1r.at[t, h, k], x_ssem.at[4 + h], a_sem.at[t % 2, k], ahead)

            for k in reversed(range(near - EARLY, near)):
                shared(k)
            for k in reversed(range(near, NZ)):
                send(s1.at[t, h, k], s1r.at[t, h, k], x_ssem.at[12], u_rsem.at[t % 2, h, k - near], across)
                send(s2.at[t, h, k], s2r.at[t, h, k], x_ssem.at[6 + h], d_sem.at[t % 2, k], ahead)
                send(plain.at[t, h, k], plainr.at[t, h, k], x_ssem.at[9 + h], p_sem.at[t % 2, 1 + k - near], behind)
            for k in reversed(range(near - EARLY)):
                shared(k)
        if near:
            at = slice(0, near)
            send(plain.at[t, 1, at], plainr.at[t, 1, at], x_ssem.at[10], q_rsem.at[t % 2, 0], right)
            send(plain.at[t, 0, at], plainr.at[t, 0, at], x_ssem.at[9], p_rsem.at[t % 2, 0], left)

        def middle(k):
            got(s1r.at[t, 0, k], a_rsem.at[t % 2, k])
            s2[t, 0, k] = (pf[0, 2, k] + s1r[t, 0, k].astype(F32)).astype(BF16)
            send(s2.at[t, 0, k], s2r.at[t, 0, k], x_ssem.at[6], d_rsem.at[t % 2, k], right)
            got(s1r.at[t, 1, k], c_rsem.at[t % 2, k])
            s2[t, 1, k] = (pf[1, 1, k] + s1r[t, 1, k].astype(F32)).astype(BF16)
            send(s2.at[t, 1, k], s2r.at[t, 1, k], x_ssem.at[7], e_rsem.at[t % 2, k], left)

        def final(k):
            to = dev(home, home_z(t, k), x, other(t))
            if k < near:
                got(s2r.at[t, 0, k], d_rsem.at[t % 2, k])
                got(s2r.at[t, 1, k], e_rsem.at[t % 2, k])
            for h in range(H):
                if k >= near:
                    got(s1r.at[t, h, k], u_rsem.at[t % 2, h, k - near])
                    got(plainr.at[t, h, k], (p_rsem if h == 0 else q_rsem).at[t % 2, 1 + k - near])
                    got(s2r.at[t, h, k], (d_rsem if h == 0 else e_rsem).at[t % 2, k])
                total = pf[h, 0, k] + s2r[t, h, k].astype(F32) + plainr[t, h, k].astype(F32)
                if k >= near:
                    total += s1r[t, h, k].astype(F32)
                eob[t, k, h] = total.astype(BF16)
                if k >= near:
                    send(eob.at[t, k, h], ret.at[t, z, h], x_ssem.at[8], r_rsem.at[t], to)
            if k < near:
                send(eob.at[t, k], ret.at[t, z], x_ssem.at[8], r_rsem.at[t], to)

        for k in reversed(range(MID, near)):
            middle(k)
        for k in reversed(range(near, NZ)):
            final(k)
        for k in reversed(range(MID)):
            middle(k)
        if near:
            got(plainr.at[t, 0, 0:near], p_rsem.at[t % 2, 0])
            got(plainr.at[t, 1, 0:near], q_rsem.at[t % 2, 0])
        for k in reversed(range(near)):
            final(k)
        before_end()
        got(ret.at[t], r_rsem.at[t])

    def experts_sent():
        sent(ag.at[:, :, 0], x_ssem.at[0])
        sent(ag.at[:, :, 0], x_ssem.at[1])
        sent(ag.at[:, 0, 1, 0:2], x_ssem.at[2])
        sent(ag.at[:, 1, 2, 0:2], x_ssem.at[3])
        sent(ag.at[0, :, 3, 2], x_ssem.at[13])
        sent(ag.at[0:2, 0, 1, 2], x_ssem.at[14])
        sent(ag.at[0:2, 1, 2, 2], x_ssem.at[15])
        sent(s1.at[:, 0, 0:near], x_ssem.at[4])
        sent(s1.at[:, 1, 0:near], x_ssem.at[5])
        sent(ag.at[:, :, 3, near:], x_ssem.at[11])
        sent(s1.at[:, :, near:], x_ssem.at[12])
        sent(s2.at[:, 0], x_ssem.at[6])
        sent(s2.at[:, 1], x_ssem.at[7])
        sent(plain.at[:, 0], x_ssem.at[9])
        sent(plain.at[:, 1], x_ssem.at[10])

    def combine(t, xref, mix, h):
        rows = returned(t, h)
        rows = jnp.concatenate([rows, rows], axis=0).astype(BF16)
        return xref[h].astype(F32) + jnp.dot(mix, rows, preferred_element_type=F32)

    def prepare(tab, xref):
        pick = chosen(tab)

        def one(h):
            pre[h] = jnp.dot(pick, xref[h], preferred_element_type=F32)

        each(one)

    def choose_rows(t, tab, tab_next):
        pick = chosen(tab_next)
        high, low = halves(tab)
        high = lax.dot_general(pick, high.astype(BF16), NT, preferred_element_type=F32)
        low = lax.dot_general(pick, low.astype(BF16), NT, preferred_element_type=F32)
        cross = jnp.concatenate([high, low], axis=0).astype(BF16)

        def one(h):
            added = jnp.dot(cross, returned(t, h).astype(BF16), preferred_element_type=F32)
            value = pre[h] + (added[0:SLOTS] + added[SLOTS:])
            rw[h] = value.astype(BF16).astype(F32)

        each(one)

    pltpu.make_async_copy(x0, x0, in_sem.at[4]).wait()
    for i, (src, dst) in enumerate(loads[2:]):
        pltpu.make_async_copy(src, dst, in_sem.at[2 + i]).wait()
    pick0 = chosen(mt[0])

    def gather(h):
        rw[h] = jnp.dot(pick0, x0[h], preferred_element_type=F32)

    for i, (src, dst) in enumerate(mats):
        pltpu.make_async_copy(src.at[0, 0], dst.at[0, c], w_sem.at[0, i]).start()
    each(gather)
    go = dispatch(0, ga, 0, True)
    pl.semaphore_wait(barrier, len(peers))
    for i, (src, dst) in enumerate(mats):
        send(src.at[0, 0], dst.at[0, c], wp_ssem.at[i], wp_rsem.at[0, i], partner)
    go()

    def background():
        send(mt.at[0], tab_a, t_ssem.at[0], t_rsem.at[0], same(2))
        send(mt.at[1], tab_b, t_ssem.at[1], t_rsem.at[1], same(1))
        send(mt.at[2], tab_c, t_ssem.at[2], t_rsem.at[2], same(1))
        send(gain.at[v1], gb, t_ssem.at[3], t_rsem.at[3], same(1))
        each(lambda h: send(x0.at[h], x1.at[h], b_ssem.at[0], b_rsem.at[0], same(2)))

        @pl.when(p < 2)
        def _():
            for i, (src, dst) in enumerate(mats):
                pltpu.make_async_copy(src.at[1, 0], dst.at[1, c], w_sem.at[1, i]).start()
                send(src.at[1, 0], dst.at[1, c], wp_ssem.at[3 + i], wp_rsem.at[1, i], partner)

    def ready1():
        got(tab_a, t_rsem.at[0])
        got(tab_b, t_rsem.at[1])
        got(gb, t_rsem.at[3])
        got(x1, b_rsem.at[0])
        prepare(tab_b[...], x1)

    def nothing():
        pass

    expert(0, 0, True, 2, nothing, background, nothing, ready1)

    choose_rows(0, tab_a[...], tab_b[...])
    dispatch(1, gb, 7, False)()

    def update1():
        mix = mixer(tab_a[...])

        def one(h):
            xs[h] = combine(0, x1, mix, h).astype(BF16)

        each(one)

    expert(1, v1, False, 1, update1, nothing, nothing, lambda: prepare(mt[2], xs))

    choose_rows(1, tab_b[...], mt[2])
    dispatch(2, gc, 0, not CROSS[2])()

    def update2():
        mix = mixer(tab_b[...])

        def one(h):
            xs2[h] = combine(1, xs, mix, h).astype(BF16)

        each(one)
        for h in range(LATE):
            send(xs2.at[h], x3.at[h], b_ssem.at[1], b_rsem.at[1], same(1))

    def ahead2():
        for h in range(LATE, H):
            send(xs2.at[h], x3.at[h], b_ssem.at[1], b_rsem.at[1], same(1))

    def ready3():
        got(tab_c, t_rsem.at[2])
        mix_c[...] = mixer(tab_c[...])
        got(x3, b_rsem.at[1])
        for t in range(TICKS):
            n = 4 if t == 1 or CROSS[t] else 3
            sent(zs.at[t, 0:n], z_ssem.at[t])
        experts_sent()
        for i, (src, dst) in enumerate(mats):
            sent(src.at[0, 0], wp_ssem.at[i])
        for i in range(3):
            sent(mt.at[i], t_ssem.at[i])
        sent(gb, t_ssem.at[3])
        sent(x0, b_ssem.at[0])
        sent(xs2, b_ssem.at[1])

        @pl.when(p < 2)
        def _():
            for i, (src, dst) in enumerate(mats):
                sent(src.at[1, 0], wp_ssem.at[3 + i])

    expert(2, v2, not CROSS[2], 1, nothing, update2, ahead2, ready3)
    def finish(h):
        out[0, :, cols(h)] = combine(2, x3, mix_c[...], h).astype(BF16)

    each(finish)
    sent(eob, x_ssem.at[8])


def per_device(acts, routes, gates, norm_gain, gate_weight, up_weight, down_weight):
    h = lambda a: pltpu.with_memory_space_constraint(a, pltpu.HBM)
    anyw = pl.BlockSpec(memory_space=pl.ANY)
    vmem = pl.BlockSpec(memory_space=pltpu.VMEM)
    V = pltpu.VMEM
    S = pltpu.SemaphoreType.DMA
    bulk = (H, TOK, DH)
    T = (SLOTS, TOK)
    scratch = [
        V((TICKS, 1, TOPK, TOK), jnp.int32), V((TICKS, 1, TOPK, TOK), F32),
        V(bulk, BF16), V(bulk, BF16), V(bulk, BF16), V(bulk, BF16), V(bulk, BF16),
        V((1, D), F32), V((1, D), F32), V((1, D), F32),
        V((TICKS, SLOTS, TOK), F32), V(T, F32), V(T, F32), V(T, F32), V((TOK, 2 * SLOTS), BF16),
        V((2, 2, D, HID), BF16), V((2, 2, D, HID), BF16), V((2, 2, HID, D), BF16),
        V((TICKS, H, NX, NZ, CAP, DH), BF16),
        V((TICKS, EXPERTS, H, CAP, DH), BF16),
        V((H, SLOTS, DH), F32), V((H, SLOTS, DH), F32),
        V((4, TOK, HID), F32),
        V((2, TOK, HID), BF16),
        V((H, 3, NZ, CAP, DH), F32),
        V((TICKS, H, NZ, CAP, DH), BF16), V((TICKS, H, NZ, CAP, DH), BF16),
        V((TICKS, H, NZ, CAP, DH), BF16), V((TICKS, H, NZ, CAP, DH), BF16),
        V((TICKS, H, NZ, CAP, DH), BF16), V((TICKS, H, NZ, CAP, DH), BF16),
        V((TICKS, NZ, H, CAP, DH), BF16),
        V((TICKS, EXPERTS, H, CAP, DH), BF16),
        S((5,)), S((2, 3)), S((6,)), S((2, 3)), S((4,)), S((4,)), S((2,)), S((2,)),
    ]
    scratch += [S((16,)), S((TICKS,)), S((TICKS, 3)), S((TICKS, 2, H)), S((2, 3)), S((2, 3)), S((2,)), S((2,))]
    scratch += [S((2, 3))] * 2 + [S((2, NZ))] * 2 + [S((2, 2))] * 2 + [S((2, 2, H)), S((2, H, 1)), S((TICKS,))]
    return pl.pallas_call(
        kernel,
        out_shape=jax.ShapeDtypeStruct((1, TOK, D), BF16),
        in_specs=[anyw, anyw, anyw, anyw, anyw, anyw, anyw],
        out_specs=vmem,
        scratch_shapes=scratch,
        compiler_params=pltpu.CompilerParams(
            collective_id=0, has_side_effects=True, vmem_limit_bytes=48 * 1024 * 1024
        ),
    )(h(acts), h(routes.transpose(0, 1, 3, 2)), h(gates.transpose(0, 1, 3, 2)), h(norm_gain), h(gate_weight), h(up_weight), h(down_weight))


def solution(mesh):
    return jax.shard_map(
        per_device,
        mesh=mesh,
        in_specs=(
            P("pipe", "expert", None),
            P(None, "pipe", "expert", None),
            P(None, "pipe", "expert", None),
            P(None, "pipe", None),
            P(None, "pipe", None, "expert"),
            P(None, "pipe", None, "expert"),
            P(None, "pipe", "expert", None),
        ),
        out_specs=P("pipe", "expert", None),
        check_vma=False,
    )
```
